256 devices in a mesh: lon: 64 (over x, z, core), lat: 4 (over y).
Axes of the slice: x: 4, y: 4, z: 8, core: 2. Of those that a mesh axis runs over, the one named last changes fastest.
Arguments:
- state: float32 [2048, 64, 1024], P('lon', None, 'lat'), may hold values from -6 to 6
Outputs:
- spectrum: float32 [2, 1024, 64, 1024], P(None, 'lon', None, 'lat')
The draws below stay inside these ranges and needn't reach their ends.
All inputs are finite; a program needn't handle non-finite values.
Results may differ from the reference program's by a relative error of at most 0.00011.
Values sent between devices are 32-bit elements; how exact they have to be, the bound alone decides.
A program may use at most 64 MiB of HBM per device.

```python
import math
import jax
import jax.numpy as jnp

NLON = 2048
FIELDS = 64
NLAT = 1024
MODES = 1024


def steps_of(rng, shape, pieces, least, top_value):
    loudness = 1.0
    for dim, blocks in pieces:
        draws = jax.random.uniform(jax.random.fold_in(jax.random.fold_in(rng, 6), dim), (blocks,), jnp.float32, least / len(pieces), top_value / len(pieces))
        loudness = loudness * jnp.repeat(jnp.exp(draws), shape[dim] // blocks).reshape((-1,) + (1,) * (len(shape) - 1 - dim))
    return loudness


def noise(rng, dims, deviation, limit, shards=(), kind=jnp.bfloat16):
    array = jax.random.normal(rng, dims, jnp.float32) * deviation
    if len(shards) > 0:
        array = steps_of(rng, dims, shards, -0.22, 0.18) * array
    return jnp.clip(array, min=-limit, max=limit).astype(kind)


def setup_inputs(seed: int = 0) -> dict:
    arg_keys = jax.random.split(jax.random.key(seed), 2)
    return {
        "state": noise(arg_keys[0], (NLON, FIELDS, NLAT), 1.0, 6.0, ((0, 64), (2, 4)), jnp.float32),
    }


def reference(state):
    spectrum = jnp.fft.rfft(state, axis=0)[:MODES] * (1.0 / math.sqrt(NLON))
    return jnp.stack([jnp.real(spectrum), jnp.imag(spectrum)]).astype(jnp.float32)
```

```python
import functools
import math

import jax
import jax.numpy as jnp
import numpy as np
from jax import lax
from jax.experimental import pallas as pl
from jax.experimental.pallas import tpu as pltpu
from jax.sharding import PartitionSpec as P

MESH = pl.DeviceIdType.MESH


def split_rows(matrix):
    high = matrix.astype(np.float32).astype(jnp.bfloat16)
    low = (matrix - high.astype(np.float64)).astype(np.float32).astype(jnp.bfloat16)
    return np.concatenate([high, low, high], axis=-1)


def tables(devices, depth):
    count, half, kept = devices * depth, devices // 2, depth // 2
    pair = np.arange(half, dtype=np.int64)
    d = np.arange(devices, dtype=np.int64)
    angle = 2.0 * math.pi / devices * (pair[:, None] * d[None, :] % devices)
    even, odd = np.cos(angle), -np.sin(angle)
    odd[0] = np.where(d % 2 == 0, 1.0, -1.0)
    first = np.concatenate([even, odd])
    j = np.arange(depth, dtype=np.int64)
    high = np.arange(kept, dtype=np.int64)
    second = np.zeros((half, 4 * kept, 2 * depth))
    scale = 1.0 / math.sqrt(count)

    def waves(low):
        turn = 2.0 * math.pi / count * ((low + devices * high)[:, None] * j[None, :] % count)
        return np.cos(turn) * scale, np.sin(turn) * scale

    for p in range(half):
        cos, sin = waves(p)
        if p == 0:
            cos_other, sin_other = waves(half)
            zero = np.zeros_like(cos)
            blocks = [[cos, zero], [-sin, zero], [zero, cos_other], [zero, -sin_other]]
        else:
            cos_other, sin_other = waves(devices - p)
            blocks = [[cos, sin], [-sin, cos], [cos_other, -sin_other], [-sin_other, -cos_other]]
        second[p] = np.block(blocks)
    return split_rows(first), split_rows(second)


def split_data(values):
    high = values.astype(jnp.bfloat16)
    low = (values - high.astype(jnp.float32)).astype(jnp.bfloat16)
    return jnp.concatenate([high, high, low], axis=0)


def kernel(
    sizes, x_hbm, first_hbm, second_hbm, out_hbm, x, g, middle, o, first, second, load_sem, send_sem, recv_sem
):
    xs, zs, cores, chunks = sizes
    devices = xs * zs * cores
    others = devices - 1
    depth, fields, lats = x_hbm.shape
    width = lats // chunks
    kept = depth // 2
    half = devices // 2

    me = lax.axis_index("lon")
    my_x, my_z, my_core = me // (zs * cores), me // cores % zs, me % cores

    def zigzag(step, size):
        odd = step % 2
        return size // 2 + (1 - odd) * (step // 2) - odd * ((step + 1) // 2)

    def peer(i):
        outer, dz = i // zs, zigzag(i % zs, zs)
        dx, dc = zigzag(outer // cores, xs), cores - 1 - outer % cores
        return (my_x + dx) % xs * (zs * cores) + (my_z + dz) % zs * cores + (my_core + dc) % cores

    load = pltpu.make_async_copy(x_hbm, x, load_sem.at[0])
    load.start()
    for chunk in range(chunks):
        lanes = pl.ds(chunk * width, width)
        pltpu.make_async_copy(x_hbm.at[:, me, lanes], g.at[:, me, lanes], recv_sem.at[0, chunk]).start()
    load_first = pltpu.make_async_copy(first_hbm, first, load_sem.at[1])
    load_first.start()
    load_second = pltpu.make_async_copy(second_hbm, second, load_sem.at[2])
    load_second.start()

    barrier = pltpu.get_barrier_semaphore()

    def greet(i, carry):
        pl.semaphore_signal(barrier, inc=1, device_id={"lon": peer(i)}, device_id_type=MESH)
        return carry

    lax.fori_loop(0, others, greet, 0)
    pl.semaphore_wait(barrier, others)
    load.wait()

    for chunk in range(chunks):
        lanes = pl.ds(chunk * width, width)

        def send_in(i, carry):
            to = peer(i)
            pltpu.make_async_remote_copy(
                src_ref=x.at[:, to, lanes],
                dst_ref=g.at[:, me, lanes],
                send_sem=send_sem.at[0],
                recv_sem=recv_sem.at[0, chunk],
                device_id={"lon": to},
                device_id_type=MESH,
            ).start()
            return carry

        lax.fori_loop(0, others, send_in, 0)

    load_first.wait()
    load_second.wait()

    for chunk in range(chunks):
        lanes = pl.ds(chunk * width, width)
        arrived = g.at[:, :, lanes]
        pltpu.make_async_copy(arrived, arrived, recv_sem.at[0, chunk]).wait()

        def stage_one(step, carry):
            matrix = first[...]
            for inner in range(2):
                j = step * 4 + inner * 2
                both = jnp.concatenate([g[j, :, lanes], g[j + 1, :, lanes]], axis=1)
                result = jnp.dot(matrix, split_data(both), preferred_element_type=jnp.float32)
                middle[pl.ds(pl.multiple_of(j * devices, devices), devices), :] = result[:, :width]
                middle[pl.ds(pl.multiple_of((j + 1) * devices, devices), devices), :] = result[:, width:]
            return carry

        lax.fori_loop(0, depth // 4, stage_one, 0)

        def stage_two(step, carry):
            for inner in range(4):
                p = step * 4 + inner
                other = (devices - p) % devices + half * ((half - 1 - p) // (half - 1))
                even = middle[pl.ds(p, depth, stride=devices), :]
                odd = middle[pl.ds(p + half, depth, stride=devices), :]
                data = split_data(jnp.concatenate([even, odd], axis=0))
                result = jnp.dot(second[p], data, preferred_element_type=jnp.float32)
                o[0, p, :, lanes] = result[:kept]
                o[1, p, :, lanes] = result[kept : 2 * kept]
                o[0, other, :, lanes] = result[2 * kept : 3 * kept]
                o[1, other, :, lanes] = result[3 * kept :]
            return carry

        lax.fori_loop(0, half // 4, stage_two, 0)

        blocks = devices // kept

        def send_out(i, carry):
            to = peer(i)
            pltpu.make_async_remote_copy(
                src_ref=o.at[:, pl.ds(to % blocks * kept, kept), to // blocks, lanes],
                dst_ref=out_hbm.at[:, :, me, lanes],
                send_sem=send_sem.at[1],
                recv_sem=recv_sem.at[1, chunk],
                device_id={"lon": to},
                device_id_type=MESH,
            ).start()
            return carry

        lax.fori_loop(0, others, send_out, 0)
        pltpu.make_async_copy(
            o.at[:, pl.ds(me % blocks * kept, kept), me // blocks, lanes],
            out_hbm.at[:, :, me, lanes],
            recv_sem.at[1, chunk],
        ).start()

    for chunk in range(chunks):
        lanes = pl.ds(chunk * width, width)
        landed = out_hbm.at[:, :, :, lanes]
        pltpu.make_async_copy(landed, landed, recv_sem.at[1, chunk]).wait()
    sent = o.at[:, pl.ds(0, others)]
    pltpu.make_async_copy(sent, sent, send_sem.at[0]).wait()
    pltpu.make_async_copy(sent, sent, send_sem.at[1]).wait()


def solution(mesh):
    devices = mesh.shape["lon"]
    sizes = (4, devices // 8, 2, 2)

    def local(state):
        depth, fields, lats = state.shape
        chunks = sizes[3]
        kept = depth // 2
        first, second = tables(devices, depth)
        return pl.pallas_call(
            functools.partial(kernel, sizes),
            out_shape=jax.ShapeDtypeStruct((2, kept, fields, lats), jnp.float32),
            in_specs=[pl.BlockSpec(memory_space=pl.ANY)] * 3,
            out_specs=pl.BlockSpec(memory_space=pl.ANY),
            scratch_shapes=[
                pltpu.VMEM((depth, fields, lats), jnp.float32),
                pltpu.VMEM((depth, devices, lats), jnp.float32),
                pltpu.VMEM((depth * devices, lats // chunks), jnp.float32),
                pltpu.VMEM((2, devices, kept, lats), jnp.float32),
                pltpu.VMEM(first.shape, jnp.bfloat16),
                pltpu.VMEM(second.shape, jnp.bfloat16),
                pltpu.SemaphoreType.DMA((3,)),
                pltpu.SemaphoreType.DMA((2,)),
                pltpu.SemaphoreType.DMA((2, chunks)),
            ],
            compiler_params=pltpu.CompilerParams(
                collective_id=0, has_side_effects=True, vmem_limit_bytes=56 * 1024 * 1024
            ),
            name="spectrum",
        )(state, jnp.asarray(first), jnp.asarray(second))

    return jax.shard_map(
        local,
        mesh=mesh,
        in_specs=(P("lon", None, "lat"),),
        out_specs=P(None, "lon", None, "lat"),
        check_vma=False,
    )
```

```python
import functools
import math

import jax
import jax.numpy as jnp
import numpy as np
from jax import lax
from jax.experimental import pallas as pl
from jax.experimental.pallas import tpu as pltpu
from jax.sharding import PartitionSpec as P

MESH = pl.DeviceIdType.MESH


def split_rows(matrix):
    high = matrix.astype(np.float32).astype(jnp.bfloat16)
    low = (matrix - high.astype(np.float64)).astype(np.float32).astype(jnp.bfloat16)
    return np.concatenate([high, low, high], axis=-1)


def tables(devices, depth):
    count, half, kept = devices * depth, devices // 2, depth // 2
    pair = np.arange(half, dtype=np.int64)
    d = np.arange(devices, dtype=np.int64)
    angle = 2.0 * math.pi / devices * (pair[:, None] * d[None, :] % devices)
    even, odd = np.cos(angle), -np.sin(angle)
    odd[0] = np.where(d % 2 == 0, 1.0, -1.0)
    first = np.concatenate([even, odd])
    j = np.arange(depth, dtype=np.int64)
    high = np.arange(kept, dtype=np.int64)
    second = np.zeros((half, 4 * kept, 2 * depth))
    scale = 1.0 / math.sqrt(count)

    def waves(low):
        turn = 2.0 * math.pi / count * ((low + devices * high)[:, None] * j[None, :] % count)
        return np.cos(turn) * scale, np.sin(turn) * scale

    for p in range(half):
        cos, sin = waves(p)
        if p == 0:
            cos_other, sin_other = waves(half)
            zero = np.zeros_like(cos)
            blocks = [[cos, zero], [-sin, zero], [zero, cos_other], [zero, -sin_other]]
        else:
            cos_other, sin_other = waves(devices - p)
            blocks = [[cos, sin], [-sin, cos], [cos_other, -sin_other], [-sin_other, -cos_other]]
        second[p] = np.block(blocks)
    return split_rows(first), split_rows(second)


def split_data(values):
    high = values.astype(jnp.bfloat16)
    low = (values - high.astype(jnp.float32)).astype(jnp.bfloat16)
    return jnp.concatenate([high, high, low], axis=0)


SEND_FROM_HBM = False
BOTH = 1
IN_ORDERS = ("near", "near")
OUT_ORDERS = ("mixback", "mixback")


def ring(step, size):
    return min(step % size, -step % size)


def arrange(shape, order):
    xs, zs, cores = shape
    offsets = [
        (dx, dz, dc)
        for dc in range(cores)
        for dx in sorted(range(xs), key=lambda d: (ring(d, xs), d))
        for dz in sorted(range(zs), key=lambda d: (ring(d, zs), d))
    ][1:]
    distance = lambda o: ring(o[0], xs) + ring(o[1], zs) + o[2]
    if order == "near":
        return sorted(offsets, key=distance)
    if order == "far":
        return sorted(offsets, key=distance, reverse=True)
    if order == "zfar":
        return sorted(offsets, key=lambda o: ring(o[1], zs), reverse=True)
    if order == "znear":
        return sorted(offsets, key=lambda o: ring(o[1], zs))
    return offsets[::-1] if order == "mixback" else offsets


def steps_away(offset, shape):
    hops = ring(offset[0], shape[0]) + ring(offset[1], shape[1])
    return max(hops, 1)


def kernel(sizes, x_hbm, first_hbm, second_hbm, out, x, g, middle, o, first, second, load_sem, send_sem, recv_sem, ready_sem):
    *shape, chunks = sizes
    xs, zs, cores = shape
    devices = xs * zs * cores
    others = devices - 1
    depth, fields, lats = x_hbm.shape
    width = lats // chunks
    kept = depth // 2
    half = devices // 2

    me = lax.axis_index("lon")
    my_x, my_z, my_core = me // (zs * cores), me // cores % zs, me % cores
    part_x = [(my_x + d) % xs * (zs * cores) for d in range(xs)]
    part_z = [(my_z + d) % zs * cores for d in range(zs)]
    part_core = [(my_core + d) % cores for d in range(cores)]

    def peer(offset):
        dx, dz, dc = offset
        return part_x[dx] + part_z[dz] + part_core[dc]

    neighbours = [n for n in arrange(shape, "near") if steps_away(n, shape) == 1]

    barrier = pltpu.get_barrier_semaphore()
    for n in neighbours:
        pl.semaphore_signal(barrier, inc=1, device_id={"lon": peer(n)}, device_id_type=MESH)

    loads = []
    for chunk in range(chunks):
        lanes = pl.ds(chunk * width, width)
        if not SEND_FROM_HBM:
            load = pltpu.make_async_copy(x_hbm.at[:, :, lanes], x.at[:, :, lanes], load_sem.at[2 + chunk])
            load.start()
            loads.append(load)
    for chunk in range(chunks):
        lanes = pl.ds(chunk * width, width)
        pltpu.make_async_copy(x_hbm.at[:, me, lanes], g.at[:, me, lanes], recv_sem.at[0, chunk]).start()
    load_first = pltpu.make_async_copy(first_hbm, first, load_sem.at[0])
    load_first.start()
    load_second = pltpu.make_async_copy(second_hbm, second, load_sem.at[1])
    load_second.start()

    def send_in(chunk, offset):
        to = peer(offset)
        lanes = pl.ds(chunk * width, width)
        pltpu.make_async_remote_copy(
            src_ref=(x_hbm if SEND_FROM_HBM else x).at[:, to, lanes],
            dst_ref=g.at[:, me, lanes],
            send_sem=send_sem.at[0],
            recv_sem=recv_sem.at[0, chunk],
            device_id={"lon": to},
            device_id_type=MESH,
        ).start()

    pl.semaphore_wait(barrier, len(neighbours))
    farthest = xs // 2 + zs // 2
    for radius in range(1, farthest + 1):
        if radius < farthest:
            for n in neighbours:
                pl.semaphore_signal(ready_sem.at[radius - 1], inc=1, device_id={"lon": peer(n)}, device_id_type=MESH)
        if radius == 1 and loads:
            loads[0].wait()
        for offset in arrange(shape, IN_ORDERS[0]):
            if steps_away(offset, shape) == radius:
                send_in(0, offset)
        if radius == BOTH and loads:
            loads[1].wait()
        if radius <= BOTH:
            for offset in arrange(shape, IN_ORDERS[0]):
                if steps_away(offset, shape) == radius:
                    send_in(1, offset)
        if radius < farthest:
            pl.semaphore_wait(ready_sem.at[radius - 1], len(neighbours))
    for chunk in range(1, chunks):
        if loads and not BOTH:
            loads[chunk].wait()
        for offset in arrange(shape, IN_ORDERS[1]):
            if steps_away(offset, shape) > BOTH:
                send_in(chunk, offset)

    load_first.wait()
    load_second.wait()

    for chunk in range(chunks):
        lanes = pl.ds(chunk * width, width)
        arrived = g.at[:, :, lanes]
        pltpu.make_async_copy(arrived, arrived, recv_sem.at[0, chunk]).wait()

        def stage_one(step, carry):
            matrix = first[...]
            for inner in range(2):
                j = step * 4 + inner * 2
                both = jnp.concatenate([g[j, :, lanes], g[j + 1, :, lanes]], axis=1)
                result = jnp.dot(matrix, split_data(both), preferred_element_type=jnp.float32)
                middle[pl.ds(pl.multiple_of(j * devices, devices), devices), :] = result[:, :width]
                middle[pl.ds(pl.multiple_of((j + 1) * devices, devices), devices), :] = result[:, width:]
            return carry

        lax.fori_loop(0, depth // 4, stage_one, 0)

        def stage_two(step, carry):
            for inner in range(4):
                p = step * 4 + inner
                other = (devices - p) % devices + half * ((half - 1 - p) // (half - 1))
                even = middle[pl.ds(p, depth, stride=devices), :]
                odd = middle[pl.ds(p + half, depth, stride=devices), :]
                data = split_data(jnp.concatenate([even, odd], axis=0))
                result = jnp.dot(second[p], data, preferred_element_type=jnp.float32)
                o[0, p, :, lanes] = result[:kept]
                o[1, p, :, lanes] = result[kept : 2 * kept]
                o[0, other, :, lanes] = result[2 * kept : 3 * kept]
                o[1, other, :, lanes] = result[3 * kept :]
            return carry

        lax.fori_loop(0, half // 4, stage_two, 0)

        blocks = devices // kept

        for offset in arrange(shape, OUT_ORDERS[chunk]):
            to = peer(offset)
            pltpu.make_async_remote_copy(
                src_ref=o.at[:, pl.ds(to % blocks * kept, kept), to // blocks, lanes],
                dst_ref=out.at[:, :, me, lanes],
                send_sem=send_sem.at[1],
                recv_sem=recv_sem.at[1, chunk],
                device_id={"lon": to},
                device_id_type=MESH,
            ).start()
        pltpu.make_async_copy(
            o.at[:, pl.ds(me % blocks * kept, kept), me // blocks, lanes],
            out.at[:, :, me, lanes],
            recv_sem.at[1, chunk],
        ).start()

    for chunk in range(chunks):
        lanes = pl.ds(chunk * width, width)
        landed = out.at[:, :, :, lanes]
        pltpu.make_async_copy(landed, landed, recv_sem.at[1, chunk]).wait()
    sent = o.at[:, pl.ds(0, others)]
    pltpu.make_async_copy(sent, sent, send_sem.at[0]).wait()
    pltpu.make_async_copy(sent, sent, send_sem.at[1]).wait()


def solution(mesh):
    devices = mesh.shape["lon"]
    sizes = (4, devices // 8, 2, 2)

    def local(state):
        depth, fields, lats = state.shape
        chunks = sizes[3]
        kept = depth // 2
        first, second = tables(devices, depth)
        return pl.pallas_call(
            functools.partial(kernel, sizes),
            out_shape=jax.ShapeDtypeStruct((2, kept, fields, lats), jnp.float32),
            in_specs=[pl.BlockSpec(memory_space=pl.ANY)] * 3,
            out_specs=pl.BlockSpec(memory_space=pltpu.VMEM),
            scratch_shapes=[
                pltpu.VMEM((depth, fields, lats), jnp.float32),
                pltpu.VMEM((depth, devices, lats), jnp.float32),
                pltpu.VMEM((depth * devices, lats // chunks), jnp.float32),
                pltpu.VMEM((2, devices, kept, lats), jnp.float32),
                pltpu.VMEM(first.shape, jnp.bfloat16),
                pltpu.VMEM(second.shape, jnp.bfloat16),
                pltpu.SemaphoreType.DMA((2 + chunks,)),
                pltpu.SemaphoreType.DMA((2,)),
                pltpu.SemaphoreType.DMA((2, chunks)),
                pltpu.SemaphoreType.REGULAR((devices // 8 + 4,)),
            ],
            compiler_params=pltpu.CompilerParams(
                collective_id=0, has_side_effects=True, vmem_limit_bytes=16 * 1024 * 1024
            ),
            name="spectrum",
        )(*(pltpu.with_memory_space_constraint(array, pltpu.HBM) for array in (state, jnp.asarray(first), jnp.asarray(second))))

    return jax.shard_map(
        local,
        mesh=mesh,
        in_specs=(P("lon", None, "lat"),),
        out_specs=P(None, "lon", None, "lat"),
        check_vma=False,
    )
```

```python
import functools
import math

import jax
import jax.numpy as jnp
import numpy as np
from jax import lax
from jax.experimental import pallas as pl
from jax.experimental.pallas import tpu as pltpu
from jax.sharding import PartitionSpec as P

MESH = pl.DeviceIdType.MESH


def split_rows(matrix):
    high = matrix.astype(np.float32).astype(jnp.bfloat16)
    low = (matrix - high.astype(np.float64)).astype(np.float32).astype(jnp.bfloat16)
    return np.concatenate([high, low, high], axis=-1)


def tables(devices, depth):
    count, half, kept = devices * depth, devices // 2, depth // 2
    pair = np.arange(half, dtype=np.int64)
    d = np.arange(devices, dtype=np.int64)
    angle = 2.0 * math.pi / devices * (pair[:, None] * d[None, :] % devices)
    even, odd = np.cos(angle), -np.sin(angle)
    odd[0] = np.where(d % 2 == 0, 1.0, -1.0)
    first = np.concatenate([even, odd])
    j = np.arange(depth, dtype=np.int64)
    high = np.arange(kept, dtype=np.int64)
    second = np.zeros((half, 4 * kept, 2 * depth))
    scale = 1.0 / math.sqrt(count)

    def waves(low):
        turn = 2.0 * math.pi / count * ((low + devices * high)[:, None] * j[None, :] % count)
        return np.cos(turn) * scale, np.sin(turn) * scale

    for p in range(half):
        cos, sin = waves(p)
        if p == 0:
            cos_other, sin_other = waves(half)
            zero = np.zeros_like(cos)
            blocks = [[cos, zero], [-sin, zero], [zero, cos_other], [zero, -sin_other]]
        else:
            cos_other, sin_other = waves(devices - p)
            blocks = [[cos, sin], [-sin, cos], [cos_other, -sin_other], [-sin_other, -cos_other]]
        second[p] = np.block(blocks)
    return split_rows(first), split_rows(second)


def split_data(values):
    high = values.astype(jnp.bfloat16)
    low = (values - high.astype(jnp.float32)).astype(jnp.bfloat16)
    return jnp.concatenate([high, high, low], axis=0)


SEND_FROM_HBM = False
BOTH = 1
WINDOW = 2
RANK = (0, 1, 2, 2, 3, 3, 3, 3)
IN_ORDERS = ("near", "end_far")
OUT_ORDERS = ("end_far", "end_far")


def ring(step, size):
    return min(step % size, -step % size)


def arrange(shape, order):
    xs, zs, cores = shape
    offsets = [
        (dx, dz, dc)
        for dc in range(cores)
        for dx in sorted(range(xs), key=lambda d: (ring(d, xs), d))
        for dz in sorted(range(zs), key=lambda d: (ring(d, zs), d))
    ][1:]
    distance = lambda o: ring(o[0], xs) + ring(o[1], zs) + o[2]
    if order == "near":
        return sorted(offsets, key=distance)
    if order == "far":
        return sorted(offsets, key=distance, reverse=True)
    if order == "zfar":
        return sorted(offsets, key=lambda o: ring(o[1], zs), reverse=True)
    if order == "znear":
        return sorted(offsets, key=lambda o: ring(o[1], zs))
    if order == "end_far":
        return sorted(offsets[::-1], key=lambda o: -ring(o[0], xs))
    return offsets[::-1] if order == "mixback" else offsets


def steps_away(offset, shape):
    hops = ring(offset[0], shape[0]) + ring(offset[1], shape[1])
    return max(hops, 1)


def ranked(shape, order, at_z):
    zs = shape[1]
    passes = list(dict.fromkeys((o[0], o[2]) for o in order))
    head = [o for o in order if (o[0], o[2]) not in passes[-WINDOW:]]
    tail = [o for o in order if (o[0], o[2]) in passes[-WINDOW:]]
    ways = [[], [], []]
    for o in tail:
        if o[1] == 0:
            ways[0].append(o)
        elif o[1] * 2 == zs:
            ways[1 + (o[0] + o[2] + at_z) % 2].append(o)
        else:
            ways[1 if o[1] * 2 < zs else 2].append(o)
    for way in ways[1:]:
        way.sort(key=lambda o: (RANK[(at_z + o[1]) % zs], -ring(o[1], zs)))
    turns = [o for pair in zip(ways[1], ways[2]) for o in pair]
    longer = max(ways[1:], key=len)
    return head + ways[0] + turns + longer[len(turns) // 2 :]


def kernel(sizes, x_hbm, first_hbm, second_hbm, out, x, g, middle, o, first, second, load_sem, send_sem, recv_sem, ready_sem):
    *shape, chunks = sizes
    xs, zs, cores = shape
    devices = xs * zs * cores
    others = devices - 1
    depth, fields, lats = x_hbm.shape
    width = lats // chunks
    kept = depth // 2
    half = devices // 2

    me = lax.axis_index("lon")
    my_x, my_z, my_core = me // (zs * cores), me // cores % zs, me % cores
    part_x = [(my_x + d) % xs * (zs * cores) for d in range(xs)]
    part_z = [(my_z + d) % zs * cores for d in range(zs)]
    part_core = [(my_core + d) % cores for d in range(cores)]

    def peer(offset):
        dx, dz, dc = offset
        return part_x[dx] + part_z[dz] + part_core[dc]

    neighbours = [n for n in arrange(shape, "near") if steps_away(n, shape) == 1]

    barrier = pltpu.get_barrier_semaphore()
    for n in neighbours:
        pl.semaphore_signal(barrier, inc=1, device_id={"lon": peer(n)}, device_id_type=MESH)

    loads = []
    for chunk in range(chunks):
        lanes = pl.ds(chunk * width, width)
        if not SEND_FROM_HBM:
            load = pltpu.make_async_copy(x_hbm.at[:, :, lanes], x.at[:, :, lanes], load_sem.at[2 + chunk])
            load.start()
            loads.append(load)
    for chunk in range(chunks):
        lanes = pl.ds(chunk * width, width)
        pltpu.make_async_copy(x_hbm.at[:, me, lanes], g.at[:, me, lanes], recv_sem.at[0, chunk]).start()
    load_first = pltpu.make_async_copy(first_hbm, first, load_sem.at[0])
    load_first.start()
    load_second = pltpu.make_async_copy(second_hbm, second, load_sem.at[1])
    load_second.start()

    def send_in(chunk, offset):
        to = peer(offset)
        lanes = pl.ds(chunk * width, width)
        pltpu.make_async_remote_copy(
            src_ref=(x_hbm if SEND_FROM_HBM else x).at[:, to, lanes],
            dst_ref=g.at[:, me, lanes],
            send_sem=send_sem.at[0],
            recv_sem=recv_sem.at[0, chunk],
            device_id={"lon": to},
            device_id_type=MESH,
        ).start()

    pl.semaphore_wait(barrier, len(neighbours))
    farthest = xs // 2 + zs // 2
    for radius in range(1, farthest + 1):
        if radius < farthest:
            for n in neighbours:
                pl.semaphore_signal(ready_sem.at[radius - 1], inc=1, device_id={"lon": peer(n)}, device_id_type=MESH)
        if radius == 1 and loads:
            loads[0].wait()
        for offset in arrange(shape, IN_ORDERS[0]):
            if steps_away(offset, shape) == radius:
                send_in(0, offset)
        if radius == BOTH and loads:
            loads[1].wait()
        if radius <= BOTH:
            for offset in arrange(shape, IN_ORDERS[0]):
                if steps_away(offset, shape) == radius:
                    send_in(1, offset)
        if radius < farthest:
            pl.semaphore_wait(ready_sem.at[radius - 1], len(neighbours))
    for chunk in range(1, chunks):
        if loads and not BOTH:
            loads[chunk].wait()
        for offset in arrange(shape, IN_ORDERS[1]):
            if steps_away(offset, shape) > BOTH:
                send_in(chunk, offset)

    load_first.wait()
    load_second.wait()

    for chunk in range(chunks):
        lanes = pl.ds(chunk * width, width)
        arrived = g.at[:, :, lanes]
        pltpu.make_async_copy(arrived, arrived, recv_sem.at[0, chunk]).wait()

        def stage_one(step, carry):
            matrix = first[...]
            for inner in range(2):
                j = step * 4 + inner * 2
                both = jnp.concatenate([g[j, :, lanes], g[j + 1, :, lanes]], axis=1)
                result = jnp.dot(matrix, split_data(both), preferred_element_type=jnp.float32)
                middle[pl.ds(pl.multiple_of(j * devices, devices), devices), :] = result[:, :width]
                middle[pl.ds(pl.multiple_of((j + 1) * devices, devices), devices), :] = result[:, width:]
            return carry

        lax.fori_loop(0, depth // 4, stage_one, 0)

        def stage_two(step, carry):
            for inner in range(4):
                p = step * 4 + inner
                other = (devices - p) % devices + half * ((half - 1 - p) // (half - 1))
                even = middle[pl.ds(p, depth, stride=devices), :]
                odd = middle[pl.ds(p + half, depth, stride=devices), :]
                data = split_data(jnp.concatenate([even, odd], axis=0))
                result = jnp.dot(second[p], data, preferred_element_type=jnp.float32)
                o[0, p, :, lanes] = result[:kept]
                o[1, p, :, lanes] = result[kept : 2 * kept]
                o[0, other, :, lanes] = result[2 * kept : 3 * kept]
                o[1, other, :, lanes] = result[3 * kept :]
            return carry

        lax.fori_loop(0, half // 4, stage_two, 0)

        blocks = devices // kept

        def send_out(offset):
            to = peer(offset)
            pltpu.make_async_remote_copy(
                src_ref=o.at[:, pl.ds(to % blocks * kept, kept), to // blocks, lanes],
                dst_ref=out.at[:, :, me, lanes],
                send_sem=send_sem.at[1],
                recv_sem=recv_sem.at[1, chunk],
                device_id={"lon": to},
                device_id_type=MESH,
            ).start()

        order = arrange(shape, OUT_ORDERS[chunk])
        if chunk < chunks - 1:
            for offset in order:
                send_out(offset)
        else:
            for at_z in range(zs):

                @pl.when(my_z == at_z)
                def _():
                    for offset in ranked(shape, order, at_z):
                        send_out(offset)

        pltpu.make_async_copy(
            o.at[:, pl.ds(me % blocks * kept, kept), me // blocks, lanes],
            out.at[:, :, me, lanes],
            recv_sem.at[1, chunk],
        ).start()

    for chunk in range(chunks):
        lanes = pl.ds(chunk * width, width)
        landed = out.at[:, :, :, lanes]
        pltpu.make_async_copy(landed, landed, recv_sem.at[1, chunk]).wait()
    sent = o.at[:, pl.ds(0, others)]
    pltpu.make_async_copy(sent, sent, send_sem.at[0]).wait()
    pltpu.make_async_copy(sent, sent, send_sem.at[1]).wait()


def solution(mesh):
    devices = mesh.shape["lon"]
    sizes = (4, devices // 8, 2, 2)

    def local(state):
        depth, fields, lats = state.shape
        chunks = sizes[3]
        kept = depth // 2
        first, second = tables(devices, depth)
        return pl.pallas_call(
            functools.partial(kernel, sizes),
            out_shape=jax.ShapeDtypeStruct((2, kept, fields, lats), jnp.float32),
            in_specs=[pl.BlockSpec(memory_space=pl.ANY)] * 3,
            out_specs=pl.BlockSpec(memory_space=pltpu.VMEM),
            scratch_shapes=[
                pltpu.VMEM((depth, fields, lats), jnp.float32),
                pltpu.VMEM((depth, devices, lats), jnp.float32),
                pltpu.VMEM((depth * devices, lats // chunks), jnp.float32),
                pltpu.VMEM((2, devices, kept, lats), jnp.float32),
                pltpu.VMEM(first.shape, jnp.bfloat16),
                pltpu.VMEM(second.shape, jnp.bfloat16),
                pltpu.SemaphoreType.DMA((2 + chunks,)),
                pltpu.SemaphoreType.DMA((2,)),
                pltpu.SemaphoreType.DMA((2, chunks)),
                pltpu.SemaphoreType.REGULAR((devices // 8 + 4,)),
            ],
            compiler_params=pltpu.CompilerParams(
                collective_id=0, has_side_effects=True, vmem_limit_bytes=16 * 1024 * 1024
            ),
            name="spectrum",
        )(*(pltpu.with_memory_space_constraint(array, pltpu.HBM) for array in (state, jnp.asarray(first), jnp.asarray(second))))

    return jax.shard_map(
        local,
        mesh=mesh,
        in_specs=(P("lon", None, "lat"),),
        out_specs=P(None, "lon", None, "lat"),
        check_vma=False,
    )
```

```python
import functools
import math

import jax
import jax.numpy as jnp
import numpy as np
from jax import lax
from jax.experimental import pallas as pl
from jax.experimental.pallas import tpu as pltpu
from jax.sharding import PartitionSpec as P

MESH = pl.DeviceIdType.MESH


def split_rows(matrix):
    high = matrix.astype(np.float32).astype(jnp.bfloat16)
    low = (matrix - high.astype(np.float64)).astype(np.float32).astype(jnp.bfloat16)
    return np.concatenate([high, low, high], axis=-1)


def tables(devices, depth):
    count, half, kept = devices * depth, devices // 2, depth // 2
    pair = np.arange(half, dtype=np.int64)
    d = np.arange(devices, dtype=np.int64)
    angle = 2.0 * math.pi / devices * (pair[:, None] * d[None, :] % devices)
    even, odd = np.cos(angle), -np.sin(angle)
    odd[0] = np.where(d % 2 == 0, 1.0, -1.0)
    first = np.concatenate([even, odd])
    j = np.arange(depth, dtype=np.int64)
    high = np.arange(kept, dtype=np.int64)
    second = np.zeros((half, 4 * kept, 2 * depth))
    scale = 1.0 / math.sqrt(count)

    def waves(low):
        turn = 2.0 * math.pi / count * ((low + devices * high)[:, None] * j[None, :] % count)
        return np.cos(turn) * scale, np.sin(turn) * scale

    for p in range(half):
        cos, sin = waves(p)
        if p == 0:
            cos_other, sin_other = waves(half)
            zero = np.zeros_like(cos)
            blocks = [[cos, zero], [-sin, zero], [zero, cos_other], [zero, -sin_other]]
        else:
            cos_other, sin_other = waves(devices - p)
            blocks = [[cos, sin], [-sin, cos], [cos_other, -sin_other], [-sin_other, -cos_other]]
        second[p] = np.block(blocks)
    return split_rows(first), split_rows(second)


def split_data(values):
    high = values.astype(jnp.bfloat16)
    low = (values - high.astype(jnp.float32)).astype(jnp.bfloat16)
    return jnp.concatenate([high, high, low], axis=0)


RANK = (0, 1, 2, 2, 3, 3, 3, 3)
LAST_PASSES = 2


def ring(step, size):
    return min(step % size, -step % size)


def hops(offset, shape):
    return max(ring(offset[0], shape[0]) + ring(offset[1], shape[1]), 1)


def offsets_of(shape):
    xs, zs, cores = shape
    return [
        (dx, dz, dc)
        for dc in range(cores)
        for dx in sorted(range(xs), key=lambda d: (ring(d, xs), d))
        for dz in sorted(range(zs), key=lambda d: (ring(d, zs), d))
    ][1:]


def near_first(shape):
    return sorted(offsets_of(shape), key=lambda o: ring(o[0], shape[0]) + ring(o[1], shape[1]) + o[2])


def far_first(shape):
    return sorted(offsets_of(shape)[::-1], key=lambda o: -ring(o[0], shape[0]))


def ranked(shape, at_z):
    zs = shape[1]
    order = far_first(shape)
    passes = list(dict.fromkeys((o[0], o[2]) for o in order))
    head = [o for o in order if (o[0], o[2]) not in passes[-LAST_PASSES:]]
    here, up, down = [], [], []
    for o in order[len(head) :]:
        if o[1] == 0:
            here.append(o)
        elif o[1] * 2 == zs:
            (down if (o[0] + o[2] + at_z) % 2 else up).append(o)
        else:
            (up if o[1] * 2 < zs else down).append(o)
    for way in (up, down):
        way.sort(key=lambda o: (RANK[(at_z + o[1]) % zs], -ring(o[1], zs)))
    turns = [o for pair in zip(up, down) for o in pair]
    longer = max((up, down), key=len)
    return head + here + turns + longer[len(turns) // 2 :]


def kernel(sizes, x_hbm, first_hbm, second_hbm, out, x, g, middle, o, first, second, load_sem, send_sem, recv_sem, ready_sem):
    *shape, chunks = sizes
    xs, zs, cores = shape
    devices = xs * zs * cores
    others = devices - 1
    depth, fields, lats = x_hbm.shape
    width = lats // chunks
    kept = depth // 2
    half = devices // 2

    me = lax.axis_index("lon")
    my_x, my_z, my_core = me // (zs * cores), me // cores % zs, me % cores
    part_x = [(my_x + d) % xs * (zs * cores) for d in range(xs)]
    part_z = [(my_z + d) % zs * cores for d in range(zs)]
    part_core = [(my_core + d) % cores for d in range(cores)]

    def peer(offset):
        dx, dz, dc = offset
        return part_x[dx] + part_z[dz] + part_core[dc]

    neighbours = [n for n in near_first(shape) if hops(n, shape) == 1]

    barrier = pltpu.get_barrier_semaphore()
    for n in neighbours:
        pl.semaphore_signal(barrier, inc=1, device_id={"lon": peer(n)}, device_id_type=MESH)

    loads = []
    for chunk in range(chunks):
        lanes = pl.ds(chunk * width, width)
        load = pltpu.make_async_copy(x_hbm.at[:, :, lanes], x.at[:, :, lanes], load_sem.at[2 + chunk])
        load.start()
        loads.append(load)
    for chunk in range(chunks):
        lanes = pl.ds(chunk * width, width)
        pltpu.make_async_copy(x_hbm.at[:, me, lanes], g.at[:, me, lanes], recv_sem.at[0, chunk]).start()
    load_first = pltpu.make_async_copy(first_hbm, first, load_sem.at[0])
    load_first.start()
    load_second = pltpu.make_async_copy(second_hbm, second, load_sem.at[1])
    load_second.start()

    def send_in(chunk, offset):
        to = peer(offset)
        lanes = pl.ds(chunk * width, width)
        pltpu.make_async_remote_copy(
            src_ref=x.at[:, to, lanes],
            dst_ref=g.at[:, me, lanes],
            send_sem=send_sem.at[0],
            recv_sem=recv_sem.at[0, chunk],
            device_id={"lon": to},
            device_id_type=MESH,
        ).start()

    pl.semaphore_wait(barrier, len(neighbours))
    farthest = xs // 2 + zs // 2
    for radius in range(1, farthest + 1):
        if radius < farthest:
            for n in neighbours:
                pl.semaphore_signal(ready_sem.at[radius - 1], inc=1, device_id={"lon": peer(n)}, device_id_type=MESH)
        for chunk in range(chunks if radius == 1 else 1):
            if radius == 1:
                loads[chunk].wait()
            for offset in near_first(shape):
                if hops(offset, shape) == radius:
                    send_in(chunk, offset)
        if radius < farthest:
            pl.semaphore_wait(ready_sem.at[radius - 1], len(neighbours))
    for chunk in range(1, chunks):
        for offset in far_first(shape):
            if hops(offset, shape) > 1:
                send_in(chunk, offset)

    load_first.wait()
    load_second.wait()

    for chunk in range(chunks):
        lanes = pl.ds(chunk * width, width)
        arrived = g.at[:, :, lanes]
        pltpu.make_async_copy(arrived, arrived, recv_sem.at[0, chunk]).wait()

        def stage_one(step, carry):
            matrix = first[...]
            for inner in range(2):
                j = step * 4 + inner * 2
                both = jnp.concatenate([g[j, :, lanes], g[j + 1, :, lanes]], axis=1)
                result = jnp.dot(matrix, split_data(both), preferred_element_type=jnp.float32)
                middle[pl.ds(pl.multiple_of(j * devices, devices), devices), :] = result[:, :width]
                middle[pl.ds(pl.multiple_of((j + 1) * devices, devices), devices), :] = result[:, width:]
            return carry

        lax.fori_loop(0, depth // 4, stage_one, 0)

        def stage_two(step, carry):
            for inner in range(4):
                p = step * 4 + inner
                other = (devices - p) % devices + half * ((half - 1 - p) // (half - 1))
                even = middle[pl.ds(p, depth, stride=devices), :]
                odd = middle[pl.ds(p + half, depth, stride=devices), :]
                data = split_data(jnp.concatenate([even, odd], axis=0))
                result = jnp.dot(second[p], data, preferred_element_type=jnp.float32)
                o[0, p, :, lanes] = result[:kept]
                o[1, p, :, lanes] = result[kept : 2 * kept]
                o[0, other, :, lanes] = result[2 * kept : 3 * kept]
                o[1, other, :, lanes] = result[3 * kept :]
            return carry

        lax.fori_loop(0, half // 4, stage_two, 0)

        blocks = devices // kept

        def send_out(offset):
            to = peer(offset)
            pltpu.make_async_remote_copy(
                src_ref=o.at[:, pl.ds(to % blocks * kept, kept), to // blocks, lanes],
                dst_ref=out.at[:, :, me, lanes],
                send_sem=send_sem.at[1],
                recv_sem=recv_sem.at[1, chunk],
                device_id={"lon": to},
                device_id_type=MESH,
            ).start()

        if chunk < chunks - 1:
            for offset in far_first(shape):
                send_out(offset)
        else:
            for at_z in range(zs):

                @pl.when(my_z == at_z)
                def _():
                    for offset in ranked(shape, at_z):
                        send_out(offset)

        pltpu.make_async_copy(
            o.at[:, pl.ds(me % blocks * kept, kept), me // blocks, lanes],
            out.at[:, :, me, lanes],
            recv_sem.at[1, chunk],
        ).start()

    for chunk in range(chunks):
        lanes = pl.ds(chunk * width, width)
        landed = out.at[:, :, :, lanes]
        pltpu.make_async_copy(landed, landed, recv_sem.at[1, chunk]).wait()
    sent = o.at[:, pl.ds(0, others)]
    pltpu.make_async_copy(sent, sent, send_sem.at[0]).wait()
    pltpu.make_async_copy(sent, sent, send_sem.at[1]).wait()


def solution(mesh):
    devices = mesh.shape["lon"]
    sizes = (4, devices // 8, 2, 2)

    def local(state):
        depth, fields, lats = state.shape
        chunks = sizes[3]
        kept = depth // 2
        first, second = tables(devices, depth)
        return pl.pallas_call(
            functools.partial(kernel, sizes),
            out_shape=jax.ShapeDtypeStruct((2, kept, fields, lats), jnp.float32),
            in_specs=[pl.BlockSpec(memory_space=pl.ANY)] * 3,
            out_specs=pl.BlockSpec(memory_space=pltpu.VMEM),
            scratch_shapes=[
                pltpu.VMEM((depth, fields, lats), jnp.float32),
                pltpu.VMEM((depth, devices, lats), jnp.float32),
                pltpu.VMEM((depth * devices, lats // chunks), jnp.float32),
                pltpu.VMEM((2, devices, kept, lats), jnp.float32),
                pltpu.VMEM(first.shape, jnp.bfloat16),
                pltpu.VMEM(second.shape, jnp.bfloat16),
                pltpu.SemaphoreType.DMA((2 + chunks,)),
                pltpu.SemaphoreType.DMA((2,)),
                pltpu.SemaphoreType.DMA((2, chunks)),
                pltpu.SemaphoreType.REGULAR((sizes[0] // 2 + sizes[1] // 2 - 1,)),
            ],
            compiler_params=pltpu.CompilerParams(
                collective_id=0, has_side_effects=True, vmem_limit_bytes=16 * 1024 * 1024
            ),
            name="spectrum",
        )(*(pltpu.with_memory_space_constraint(array, pltpu.HBM) for array in (state, jnp.asarray(first), jnp.asarray(second))))

    return jax.shard_map(
        local,
        mesh=mesh,
        in_specs=(P("lon", None, "lat"),),
        out_specs=P(None, "lon", None, "lat"),
        check_vma=False,
    )
```

```python
import functools
import math

import jax
import jax.numpy as jnp
import numpy as np
from jax import lax
from jax.experimental import pallas as pl
from jax.experimental.pallas import tpu as pltpu
from jax.sharding import PartitionSpec as P

MESH = pl.DeviceIdType.MESH


def split_rows(matrix):
    high = matrix.astype(np.float32).astype(jnp.bfloat16)
    low = (matrix - high.astype(np.float64)).astype(np.float32).astype(jnp.bfloat16)
    return np.concatenate([high, low, high], axis=-1)


def tables(devices, depth):
    count, half, kept = devices * depth, devices // 2, depth // 2
    pair = np.arange(half, dtype=np.int64)
    d = np.arange(devices, dtype=np.int64)
    angle = 2.0 * math.pi / devices * (pair[:, None] * d[None, :] % devices)
    even, odd = np.cos(angle), -np.sin(angle)
    odd[0] = np.where(d % 2 == 0, 1.0, -1.0)
    first = np.concatenate([even, odd])
    j = np.arange(depth, dtype=np.int64)
    high = np.arange(kept, dtype=np.int64)
    second = np.zeros((half, 4 * kept, 2 * depth))
    scale = 1.0 / math.sqrt(count)

    def waves(low):
        turn = 2.0 * math.pi / count * ((low + devices * high)[:, None] * j[None, :] % count)
        return np.cos(turn) * scale, np.sin(turn) * scale

    for p in range(half):
        cos, sin = waves(p)
        if p == 0:
            cos_other, sin_other = waves(half)
            zero = np.zeros_like(cos)
            blocks = [[cos, zero], [-sin, zero], [zero, cos_other], [zero, -sin_other]]
        else:
            cos_other, sin_other = waves(devices - p)
            blocks = [[cos, sin], [-sin, cos], [cos_other, -sin_other], [-sin_other, -cos_other]]
        second[p] = np.block(blocks)
    return split_rows(first), split_rows(second)


def split_data(values):
    high = values.astype(jnp.bfloat16)
    low = (values - high.astype(jnp.float32)).astype(jnp.bfloat16)
    return jnp.concatenate([high, high, low], axis=0)


RANK = (0, 1, 2, 2, 3, 3, 3, 3)
LAST_PASSES = 2


def ring(step, size):
    return min(step % size, -step % size)


def hops(offset, shape):
    flip = offset[2] if offset[1] == 0 else 0
    return ring(offset[0], shape[0]) + ring(offset[1], shape[1]) + flip


def offsets_of(shape):
    xs, zs, cores = shape
    return [
        (dx, dz, dc)
        for dc in range(cores)
        for dx in sorted(range(xs), key=lambda d: (ring(d, xs), d))
        for dz in sorted(range(zs), key=lambda d: (ring(d, zs), d))
    ][1:]


def near_first(shape):
    return sorted(offsets_of(shape), key=lambda o: ring(o[0], shape[0]) + ring(o[1], shape[1]) + o[2])


def far_first(shape):
    return sorted(offsets_of(shape)[::-1], key=lambda o: -ring(o[0], shape[0]))


def ranked(shape, at_z):
    zs = shape[1]
    order = far_first(shape)
    passes = list(dict.fromkeys((o[0], o[2]) for o in order))
    head = [o for o in order if (o[0], o[2]) not in passes[-LAST_PASSES:]]
    here, up, down = [], [], []
    for o in order[len(head) :]:
        if o[1] == 0:
            here.append(o)
        elif o[1] * 2 == zs:
            (down if (o[0] + o[2] + at_z) % 2 else up).append(o)
        else:
            (up if o[1] * 2 < zs else down).append(o)
    for way in (up, down):
        way.sort(key=lambda o: (RANK[(at_z + o[1]) % zs], -ring(o[1], zs)))
    turns = [o for pair in zip(up, down) for o in pair]
    longer = max((up, down), key=len)
    return head + here + turns + longer[len(turns) // 2 :]


def kernel(sizes, x_hbm, first_hbm, second_hbm, out, x, g, middle, o, first, second, load_sem, send_sem, recv_sem, ready_sem):
    *shape, chunks = sizes
    xs, zs, cores = shape
    devices = xs * zs * cores
    others = devices - 1
    depth, fields, lats = x_hbm.shape
    width = lats // chunks
    kept = depth // 2
    half = devices // 2

    me = lax.axis_index("lon")
    my_x, my_z, my_core = me // (zs * cores), me // cores % zs, me % cores
    part_x = [(my_x + d) % xs * (zs * cores) for d in range(xs)]
    part_z = [(my_z + d) % zs * cores for d in range(zs)]
    part_core = [(my_core + d) % cores for d in range(cores)]

    def peer(offset):
        dx, dz, dc = offset
        return part_x[dx] + part_z[dz] + part_core[dc]

    neighbours = [n for n in near_first(shape) if hops(n, shape) == 1]

    barrier = pltpu.get_barrier_semaphore()
    for n in neighbours:
        pl.semaphore_signal(barrier, inc=1, device_id={"lon": peer(n)}, device_id_type=MESH)

    loads = []
    for chunk in range(chunks):
        lanes = pl.ds(chunk * width, width)
        load = pltpu.make_async_copy(x_hbm.at[:, :, lanes], x.at[:, :, lanes], load_sem.at[2 + chunk])
        load.start()
        loads.append(load)
    for chunk in range(chunks):
        lanes = pl.ds(chunk * width, width)
        pltpu.make_async_copy(x_hbm.at[:, me, lanes], g.at[:, me, lanes], recv_sem.at[0, chunk]).start()
    load_first = pltpu.make_async_copy(first_hbm, first, load_sem.at[0])
    load_first.start()
    load_second = pltpu.make_async_copy(second_hbm, second, load_sem.at[1])
    load_second.start()

    def send_in(chunk, offset):
        to = peer(offset)
        lanes = pl.ds(chunk * width, width)
        pltpu.make_async_remote_copy(
            src_ref=x.at[:, to, lanes],
            dst_ref=g.at[:, me, lanes],
            send_sem=send_sem.at[0],
            recv_sem=recv_sem.at[0, chunk],
            device_id={"lon": to},
            device_id_type=MESH,
        ).start()

    pl.semaphore_wait(barrier, len(neighbours))
    farthest = xs // 2 + zs // 2
    for radius in range(1, farthest + 1):
        if radius < farthest:
            for n in neighbours:
                pl.semaphore_signal(ready_sem.at[radius - 1], inc=1, device_id={"lon": peer(n)}, device_id_type=MESH)
        for chunk in range(chunks if radius == 1 else 1):
            if radius == 1:
                loads[chunk].wait()
            for offset in near_first(shape):
                if hops(offset, shape) == radius:
                    send_in(chunk, offset)
        if radius < farthest:
            pl.semaphore_wait(ready_sem.at[radius - 1], len(neighbours))
    for chunk in range(1, chunks):
        for offset in far_first(shape):
            if hops(offset, shape) > 1:
                send_in(chunk, offset)

    load_first.wait()
    load_second.wait()

    for chunk in range(chunks):
        lanes = pl.ds(chunk * width, width)
        arrived = g.at[:, :, lanes]
        pltpu.make_async_copy(arrived, arrived, recv_sem.at[0, chunk]).wait()

        def stage_one(step, carry):
            matrix = first[...]
            for inner in range(2):
                j = step * 4 + inner * 2
                both = jnp.concatenate([g[j, :, lanes], g[j + 1, :, lanes]], axis=1)
                result = jnp.dot(matrix, split_data(both), preferred_element_type=jnp.float32)
                middle[pl.ds(pl.multiple_of(j * devices, devices), devices), :] = result[:, :width]
                middle[pl.ds(pl.multiple_of((j + 1) * devices, devices), devices), :] = result[:, width:]
            return carry

        lax.fori_loop(0, depth // 4, stage_one, 0)

        def stage_two(step, carry):
            for inner in range(4):
                p = step * 4 + inner
                other = (devices - p) % devices + half * ((half - 1 - p) // (half - 1))
                even = middle[pl.ds(p, depth, stride=devices), :]
                odd = middle[pl.ds(p + half, depth, stride=devices), :]
                data = split_data(jnp.concatenate([even, odd], axis=0))
                result = jnp.dot(second[p], data, preferred_element_type=jnp.float32)
                o[0, p, :, lanes] = result[:kept]
                o[1, p, :, lanes] = result[kept : 2 * kept]
                o[0, other, :, lanes] = result[2 * kept : 3 * kept]
                o[1, other, :, lanes] = result[3 * kept :]
            return carry

        lax.fori_loop(0, half // 4, stage_two, 0)

        blocks = devices // kept

        def send_out(offset):
            to = peer(offset)
            pltpu.make_async_remote_copy(
                src_ref=o.at[:, pl.ds(to % blocks * kept, kept), to // blocks, lanes],
                dst_ref=out.at[:, :, me, lanes],
                send_sem=send_sem.at[1],
                recv_sem=recv_sem.at[1, chunk],
                device_id={"lon": to},
                device_id_type=MESH,
            ).start()

        if chunk < chunks - 1:
            for offset in far_first(shape):
                send_out(offset)
        else:
            for at_z in range(zs):

                @pl.when(my_z == at_z)
                def _():
                    for offset in ranked(shape, at_z):
                        send_out(offset)

        pltpu.make_async_copy(
            o.at[:, pl.ds(me % blocks * kept, kept), me // blocks, lanes],
            out.at[:, :, me, lanes],
            recv_sem.at[1, chunk],
        ).start()

    for chunk in range(chunks):
        lanes = pl.ds(chunk * width, width)
        landed = out.at[:, :, :, lanes]
        pltpu.make_async_copy(landed, landed, recv_sem.at[1, chunk]).wait()
    sent = o.at[:, pl.ds(0, others)]
    pltpu.make_async_copy(sent, sent, send_sem.at[0]).wait()
    pltpu.make_async_copy(sent, sent, send_sem.at[1]).wait()


def solution(mesh):
    devices = mesh.shape["lon"]
    sizes = (4, devices // 8, 2, 2)

    def local(state):
        depth, fields, lats = state.shape
        chunks = sizes[3]
        kept = depth // 2
        first, second = tables(devices, depth)
        return pl.pallas_call(
            functools.partial(kernel, sizes),
            out_shape=jax.ShapeDtypeStruct((2, kept, fields, lats), jnp.float32),
            in_specs=[pl.BlockSpec(memory_space=pl.ANY)] * 3,
            out_specs=pl.BlockSpec(memory_space=pltpu.VMEM),
            scratch_shapes=[
                pltpu.VMEM((depth, fields, lats), jnp.float32),
                pltpu.VMEM((depth, devices, lats), jnp.float32),
                pltpu.VMEM((depth * devices, lats // chunks), jnp.float32),
                pltpu.VMEM((2, devices, kept, lats), jnp.float32),
                pltpu.VMEM(first.shape, jnp.bfloat16),
                pltpu.VMEM(second.shape, jnp.bfloat16),
                pltpu.SemaphoreType.DMA((2 + chunks,)),
                pltpu.SemaphoreType.DMA((2,)),
                pltpu.SemaphoreType.DMA((2, chunks)),
                pltpu.SemaphoreType.REGULAR((sizes[0] // 2 + sizes[1] // 2 - 1,)),
            ],
            compiler_params=pltpu.CompilerParams(
                collective_id=0, has_side_effects=True, vmem_limit_bytes=16 * 1024 * 1024
            ),
            name="spectrum",
        )(*(pltpu.with_memory_space_constraint(array, pltpu.HBM) for array in (state, jnp.asarray(first), jnp.asarray(second))))

    return jax.shard_map(
        local,
        mesh=mesh,
        in_specs=(P("lon", None, "lat"),),
        out_specs=P(None, "lon", None, "lat"),
        check_vma=False,
    )
```

```python
import functools
import math

import jax
import jax.numpy as jnp
import numpy as np
from jax import lax
from jax.experimental import pallas as pl
from jax.experimental.pallas import tpu as pltpu
from jax.sharding import PartitionSpec as P

MESH = pl.DeviceIdType.MESH


def split_rows(matrix):
    high = matrix.astype(np.float32).astype(jnp.bfloat16)
    low = (matrix - high.astype(np.float64)).astype(np.float32).astype(jnp.bfloat16)
    return np.concatenate([high, low, high], axis=-1)


def tables(devices, depth):
    count, half, kept = devices * depth, devices // 2, depth // 2
    pair = np.arange(half, dtype=np.int64)
    d = np.arange(devices, dtype=np.int64)
    angle = 2.0 * math.pi / devices * (pair[:, None] * d[None, :] % devices)
    even, odd = np.cos(angle), -np.sin(angle)
    odd[0] = np.where(d % 2 == 0, 1.0, -1.0)
    first = np.concatenate([even, odd])
    j = np.arange(depth, dtype=np.int64)
    high = np.arange(kept, dtype=np.int64)
    second = np.zeros((half, 4 * kept, 2 * depth))
    scale = 1.0 / math.sqrt(count)

    def waves(low):
        turn = 2.0 * math.pi / count * ((low + devices * high)[:, None] * j[None, :] % count)
        return np.cos(turn) * scale, np.sin(turn) * scale

    for p in range(half):
        cos, sin = waves(p)
        if p == 0:
            cos_other, sin_other = waves(half)
            zero = np.zeros_like(cos)
            blocks = [[cos, zero], [-sin, zero], [zero, cos_other], [zero, -sin_other]]
        else:
            cos_other, sin_other = waves(devices - p)
            blocks = [[cos, sin], [-sin, cos], [cos_other, -sin_other], [-sin_other, -cos_other]]
        second[p] = np.block(blocks)
    return split_rows(first), split_rows(second)


def split_data(values):
    high = values.astype(jnp.bfloat16)
    low = (values - high.astype(jnp.float32)).astype(jnp.bfloat16)
    return jnp.concatenate([high, high, low], axis=0)


RANK = (0, 1, 2, 2, 3, 3, 3, 3)
LAST_PASSES = 2


def ring(step, size):
    return min(step % size, -step % size)


def hops(offset, shape):
    flip = offset[2] if offset[1] == 0 else 0
    return ring(offset[0], shape[0]) + ring(offset[1], shape[1]) + flip


def offsets_of(shape):
    xs, zs, cores = shape
    return [
        (dx, dz, dc)
        for dc in range(cores)
        for dx in sorted(range(xs), key=lambda d: (ring(d, xs), d))
        for dz in sorted(range(zs), key=lambda d: (ring(d, zs), d))
    ][1:]


def near_first(shape):
    return sorted(offsets_of(shape), key=lambda o: ring(o[0], shape[0]) + ring(o[1], shape[1]) + o[2])


def far_first(shape):
    return sorted(offsets_of(shape)[::-1], key=lambda o: -ring(o[0], shape[0]))


def ranked(shape, at_z):
    zs = shape[1]
    order = far_first(shape)
    passes = list(dict.fromkeys((o[0], o[2]) for o in order))
    head = [o for o in order if (o[0], o[2]) not in passes[-LAST_PASSES:]]
    here, up, down = [], [], []
    for o in order[len(head) :]:
        if o[1] == 0:
            here.append(o)
        elif o[1] * 2 == zs:
            (up if (o[0] + o[2] + at_z) % 2 else down).append(o)
        else:
            (up if o[1] * 2 < zs else down).append(o)
    for way in (up, down):
        way.sort(key=lambda o: (RANK[(at_z + o[1]) % zs], -ring(o[1], zs)))
    if up and down and RANK[(at_z + down[0][1]) % zs] < RANK[(at_z + up[0][1]) % zs]:
        up, down = down, up
    turns = [o for pair in zip(up, down) for o in pair]
    longer = max((up, down), key=len)
    return head + here + turns + longer[len(turns) // 2 :]


def kernel(sizes, x_hbm, first_hbm, second_hbm, out, x, g, middle, o, first, second, load_sem, send_sem, recv_sem, ready_sem):
    *shape, chunks = sizes
    xs, zs, cores = shape
    devices = xs * zs * cores
    others = devices - 1
    depth, fields, lats = x_hbm.shape
    width = lats // chunks
    kept = depth // 2
    half = devices // 2

    me = lax.axis_index("lon")
    my_x, my_z, my_core = me // (zs * cores), me // cores % zs, me % cores
    part_x = [(my_x + d) % xs * (zs * cores) for d in range(xs)]
    part_z = [(my_z + d) % zs * cores for d in range(zs)]
    part_core = [(my_core + d) % cores for d in range(cores)]

    def peer(offset):
        dx, dz, dc = offset
        return part_x[dx] + part_z[dz] + part_core[dc]

    neighbours = [n for n in near_first(shape) if hops(n, shape) == 1]

    barrier = pltpu.get_barrier_semaphore()
    for n in neighbours:
        pl.semaphore_signal(barrier, inc=1, device_id={"lon": peer(n)}, device_id_type=MESH)

    loads = []
    for chunk in range(chunks):
        lanes = pl.ds(chunk * width, width)
        load = pltpu.make_async_copy(x_hbm.at[:, :, lanes], x.at[:, :, lanes], load_sem.at[2 + chunk])
        load.start()
        loads.append(load)
    for chunk in range(chunks):
        lanes = pl.ds(chunk * width, width)
        pltpu.make_async_copy(x_hbm.at[:, me, lanes], g.at[:, me, lanes], recv_sem.at[0, chunk]).start()
    load_first = pltpu.make_async_copy(first_hbm, first, load_sem.at[0])
    load_first.start()
    load_second = pltpu.make_async_copy(second_hbm, second, load_sem.at[1])
    load_second.start()

    def send_in(chunk, offset):
        to = peer(offset)
        lanes = pl.ds(chunk * width, width)
        pltpu.make_async_remote_copy(
            src_ref=x.at[:, to, lanes],
            dst_ref=g.at[:, me, lanes],
            send_sem=send_sem.at[0],
            recv_sem=recv_sem.at[0, chunk],
            device_id={"lon": to},
            device_id_type=MESH,
        ).start()

    pl.semaphore_wait(barrier, len(neighbours))
    farthest = xs // 2 + zs // 2
    for radius in range(1, farthest + 1):
        if radius < farthest:
            for n in neighbours:
                pl.semaphore_signal(ready_sem.at[radius - 1], inc=1, device_id={"lon": peer(n)}, device_id_type=MESH)
        for chunk in range(chunks if radius == 1 else 1):
            if radius == 1:
                loads[chunk].wait()
            for offset in near_first(shape):
                if hops(offset, shape) == radius:
                    send_in(chunk, offset)
        if radius < farthest:
            pl.semaphore_wait(ready_sem.at[radius - 1], len(neighbours))
    for chunk in range(1, chunks):
        for offset in far_first(shape):
            if hops(offset, shape) > 1:
                send_in(chunk, offset)

    load_first.wait()
    load_second.wait()

    for chunk in range(chunks):
        lanes = pl.ds(chunk * width, width)
        arrived = g.at[:, :, lanes]
        pltpu.make_async_copy(arrived, arrived, recv_sem.at[0, chunk]).wait()

        def stage_one(step, carry):
            matrix = first[...]
            for inner in range(2):
                j = step * 4 + inner * 2
                both = jnp.concatenate([g[j, :, lanes], g[j + 1, :, lanes]], axis=1)
                result = jnp.dot(matrix, split_data(both), preferred_element_type=jnp.float32)
                middle[pl.ds(pl.multiple_of(j * devices, devices), devices), :] = result[:, :width]
                middle[pl.ds(pl.multiple_of((j + 1) * devices, devices), devices), :] = result[:, width:]
            return carry

        lax.fori_loop(0, depth // 4, stage_one, 0)

        def stage_two(step, carry):
            for inner in range(4):
                p = step * 4 + inner
                other = (devices - p) % devices + half * ((half - 1 - p) // (half - 1))
                even = middle[pl.ds(p, depth, stride=devices), :]
                odd = middle[pl.ds(p + half, depth, stride=devices), :]
                data = split_data(jnp.concatenate([even, odd], axis=0))
                result = jnp.dot(second[p], data, preferred_element_type=jnp.float32)
                o[0, p, :, lanes] = result[:kept]
                o[1, p, :, lanes] = result[kept : 2 * kept]
                o[0, other, :, lanes] = result[2 * kept : 3 * kept]
                o[1, other, :, lanes] = result[3 * kept :]
            return carry

        lax.fori_loop(0, half // 4, stage_two, 0)

        blocks = devices // kept

        def send_out(offset):
            to = peer(offset)
            pltpu.make_async_remote_copy(
                src_ref=o.at[:, pl.ds(to % blocks * kept, kept), to // blocks, lanes],
                dst_ref=out.at[:, :, me, lanes],
                send_sem=send_sem.at[1],
                recv_sem=recv_sem.at[1, chunk],
                device_id={"lon": to},
                device_id_type=MESH,
            ).start()

        if chunk < chunks - 1:
            for offset in far_first(shape):
                send_out(offset)
        else:
            for at_z in range(zs):

                @pl.when(my_z == at_z)
                def _():
                    for offset in ranked(shape, at_z):
                        send_out(offset)

        pltpu.make_async_copy(
            o.at[:, pl.ds(me % blocks * kept, kept), me // blocks, lanes],
            out.at[:, :, me, lanes],
            recv_sem.at[1, chunk],
        ).start()

    for chunk in range(chunks):
        lanes = pl.ds(chunk * width, width)
        landed = out.at[:, :, :, lanes]
        pltpu.make_async_copy(landed, landed, recv_sem.at[1, chunk]).wait()
    sent = o.at[:, pl.ds(0, others)]
    pltpu.make_async_copy(sent, sent, send_sem.at[0]).wait()
    pltpu.make_async_copy(sent, sent, send_sem.at[1]).wait()


def solution(mesh):
    devices = mesh.shape["lon"]
    sizes = (4, devices // 8, 2, 2)

    def local(state):
        depth, fields, lats = state.shape
        chunks = sizes[3]
        kept = depth // 2
        first, second = tables(devices, depth)
        return pl.pallas_call(
            functools.partial(kernel, sizes),
            out_shape=jax.ShapeDtypeStruct((2, kept, fields, lats), jnp.float32),
            in_specs=[pl.BlockSpec(memory_space=pl.ANY)] * 3,
            out_specs=pl.BlockSpec(memory_space=pltpu.VMEM),
            scratch_shapes=[
                pltpu.VMEM((depth, fields, lats), jnp.float32),
                pltpu.VMEM((depth, devices, lats), jnp.float32),
                pltpu.VMEM((depth * devices, lats // chunks), jnp.float32),
                pltpu.VMEM((2, devices, kept, lats), jnp.float32),
                pltpu.VMEM(first.shape, jnp.bfloat16),
                pltpu.VMEM(second.shape, jnp.bfloat16),
                pltpu.SemaphoreType.DMA((2 + chunks,)),
                pltpu.SemaphoreType.DMA((2,)),
                pltpu.SemaphoreType.DMA((2, chunks)),
                pltpu.SemaphoreType.REGULAR((sizes[0] // 2 + sizes[1] // 2 - 1,)),
            ],
            compiler_params=pltpu.CompilerParams(
                collective_id=0, has_side_effects=True, vmem_limit_bytes=16 * 1024 * 1024
            ),
            name="spectrum",
        )(*(pltpu.with_memory_space_constraint(array, pltpu.HBM) for array in (state, jnp.asarray(first), jnp.asarray(second))))

    return jax.shard_map(
        local,
        mesh=mesh,
        in_specs=(P("lon", None, "lat"),),
        out_specs=P(None, "lon", None, "lat"),
        check_vma=False,
    )
```

```python
import functools
import math

import jax
import jax.numpy as jnp
import numpy as np
from jax import lax
from jax.experimental import pallas as pl
from jax.experimental.pallas import tpu as pltpu
from jax.sharding import PartitionSpec as P

MESH = pl.DeviceIdType.MESH


def split_rows(matrix):
    high = matrix.astype(np.float32).astype(jnp.bfloat16)
    low = (matrix - high.astype(np.float64)).astype(np.float32).astype(jnp.bfloat16)
    return np.concatenate([high, low, high], axis=-1)


def tables(devices, depth):
    count, half, kept = devices * depth, devices // 2, depth // 2
    pair = np.arange(half, dtype=np.int64)
    d = np.arange(devices, dtype=np.int64)
    angle = 2.0 * math.pi / devices * (pair[:, None] * d[None, :] % devices)
    even, odd = np.cos(angle), -np.sin(angle)
    odd[0] = np.where(d % 2 == 0, 1.0, -1.0)
    first = np.concatenate([even, odd])
    j = np.arange(depth, dtype=np.int64)
    high = np.arange(kept, dtype=np.int64)
    second = np.zeros((half, 4 * kept, 2 * depth))
    scale = 1.0 / math.sqrt(count)

    def waves(low):
        turn = 2.0 * math.pi / count * ((low + devices * high)[:, None] * j[None, :] % count)
        return np.cos(turn) * scale, np.sin(turn) * scale

    for p in range(half):
        cos, sin = waves(p)
        if p == 0:
            cos_other, sin_other = waves(half)
            zero = np.zeros_like(cos)
            blocks = [[cos, zero], [-sin, zero], [zero, cos_other], [zero, -sin_other]]
        else:
            cos_other, sin_other = waves(devices - p)
            blocks = [[cos, sin], [-sin, cos], [cos_other, -sin_other], [-sin_other, -cos_other]]
        second[p] = np.block(blocks)
    return split_rows(first), split_rows(second)


def split_data(values):
    high = values.astype(jnp.bfloat16)
    low = (values - high.astype(jnp.float32)).astype(jnp.bfloat16)
    return jnp.concatenate([high, high, low], axis=0)


RANK = (0, 1, 2, 2, 3, 3, 3, 3)
LAST_PASSES = 2


def ring(step, size):
    return min(step % size, -step % size)


def hops(offset, shape):
    flip = offset[2] if offset[1] == 0 else 0
    return ring(offset[0], shape[0]) + ring(offset[1], shape[1]) + flip


def offsets_of(shape):
    xs, zs, cores = shape
    return [
        (dx, dz, dc)
        for dc in range(cores)
        for dx in sorted(range(xs), key=lambda d: (ring(d, xs), d))
        for dz in sorted(range(zs), key=lambda d: (ring(d, zs), d))
    ][1:]


def near_first(shape):
    return sorted(offsets_of(shape), key=lambda o: ring(o[0], shape[0]) + ring(o[1], shape[1]) + o[2])


def far_first(shape):
    return sorted(offsets_of(shape)[::-1], key=lambda o: -ring(o[0], shape[0]))


def ranked(shape, at_z):
    zs = shape[1]
    order = far_first(shape)
    passes = list(dict.fromkeys((o[0], o[2]) for o in order))
    head = [o for o in order if (o[0], o[2]) not in passes[-LAST_PASSES:]]
    here, up, down = [], [], []
    for o in order[len(head) :]:
        if o[1] == 0:
            here.append(o)
        elif o[1] * 2 == zs:
            (up if (o[0] + o[2] + at_z) % 2 else down).append(o)
        else:
            (up if o[1] * 2 < zs else down).append(o)
    for way in (up, down):
        way.sort(key=lambda o: (RANK[(at_z + o[1]) % zs], -ring(o[1], zs)))
    if up and down and RANK[(at_z + down[0][1]) % zs] < RANK[(at_z + up[0][1]) % zs]:
        up, down = down, up
    turns = [o for pair in zip(up, down) for o in pair]
    longer = max((up, down), key=len)
    return head + here + turns + longer[len(turns) // 2 :]


def kernel(sizes, x_hbm, first_hbm, second_hbm, out, x, g, middle, o, first, second, load_sem, send_sem, recv_sem, ready_sem):
    *shape, chunks = sizes
    xs, zs, cores = shape
    devices = xs * zs * cores
    others = devices - 1
    depth, fields, lats = x_hbm.shape
    width = lats // chunks
    kept = depth // 2
    half = devices // 2

    me = lax.axis_index("lon")
    my_x, my_z, my_core = me // (zs * cores), me // cores % zs, me % cores
    part_x = [(my_x + d) % xs * (zs * cores) for d in range(xs)]
    part_z = [(my_z + d) % zs * cores for d in range(zs)]
    part_core = [(my_core + d) % cores for d in range(cores)]

    def peer(offset):
        dx, dz, dc = offset
        return part_x[dx] + part_z[dz] + part_core[dc]

    neighbours = [n for n in near_first(shape) if hops(n, shape) == 1]

    barrier = pltpu.get_barrier_semaphore()
    for n in neighbours:
        pl.semaphore_signal(barrier, inc=1, device_id={"lon": peer(n)}, device_id_type=MESH)

    loads = []
    for chunk in range(chunks):
        lanes = pl.ds(chunk * width, width)
        load = pltpu.make_async_copy(x_hbm.at[:, :, lanes], x.at[:, :, lanes], load_sem.at[2 + chunk])
        load.start()
        loads.append(load)
    for chunk in range(chunks):
        lanes = pl.ds(chunk * width, width)
        pltpu.make_async_copy(x_hbm.at[:, me, lanes], g.at[:, me, lanes], recv_sem.at[0, chunk]).start()
    load_first = pltpu.make_async_copy(first_hbm, first, load_sem.at[0])
    load_first.start()
    load_second = pltpu.make_async_copy(second_hbm, second, load_sem.at[1])
    load_second.start()

    def send_in(chunk, offset):
        to = peer(offset)
        lanes = pl.ds(chunk * width, width)
        pltpu.make_async_remote_copy(
            src_ref=x.at[:, to, lanes],
            dst_ref=g.at[:, me, lanes],
            send_sem=send_sem.at[0],
            recv_sem=recv_sem.at[0, chunk],
            device_id={"lon": to},
            device_id_type=MESH,
        ).start()

    pl.semaphore_wait(barrier, len(neighbours))
    farthest = xs // 2 + zs // 2
    for radius in range(1, farthest + 1):
        if radius < farthest:
            for n in neighbours:
                pl.semaphore_signal(ready_sem.at[radius - 1], inc=1, device_id={"lon": peer(n)}, device_id_type=MESH)
        for chunk in range(chunks if radius == 1 else 1):
            if radius == 1:
                loads[chunk].wait()
            for offset in near_first(shape):
                if hops(offset, shape) == radius:
                    send_in(chunk, offset)
        if radius < farthest:
            pl.semaphore_wait(ready_sem.at[radius - 1], len(neighbours))
    for chunk in range(1, chunks):
        for offset in far_first(shape):
            if hops(offset, shape) > 1:
                send_in(chunk, offset)

    load_first.wait()
    load_second.wait()

    for chunk in range(chunks):
        lanes = pl.ds(chunk * width, width)
        arrived = g.at[:, :, lanes]
        pltpu.make_async_copy(arrived, arrived, recv_sem.at[0, chunk]).wait()

        def stage_one(step, carry):
            matrix = first[...]
            for inner in range(2):
                j = step * 4 + inner * 2
                both = jnp.concatenate([g[j, :, lanes], g[j + 1, :, lanes]], axis=1)
                result = jnp.dot(matrix, split_data(both), preferred_element_type=jnp.float32)
                middle[pl.ds(pl.multiple_of(j * devices, devices), devices), :] = result[:, :width]
                middle[pl.ds(pl.multiple_of((j + 1) * devices, devices), devices), :] = result[:, width:]
            return carry

        lax.fori_loop(0, depth // 4, stage_one, 0)

        def stage_two(step, carry):
            for inner in range(4):
                p = step * 4 + inner
                other = (devices - p) % devices + half * ((half - 1 - p) // (half - 1))
                even = middle[pl.ds(p, depth, stride=devices), :]
                odd = middle[pl.ds(p + half, depth, stride=devices), :]
                data = split_data(jnp.concatenate([even, odd], axis=0))
                result = jnp.dot(second[p], data, preferred_element_type=jnp.float32)
                o[0, p, :, lanes] = result[:kept]
                o[1, p, :, lanes] = result[kept : 2 * kept]
                o[0, other, :, lanes] = result[2 * kept : 3 * kept]
                o[1, other, :, lanes] = result[3 * kept :]
            return carry

        lax.fori_loop(0, half // 4, stage_two, 0)

        blocks = devices // kept

        def send_out(offset):
            to = peer(offset)
            pltpu.make_async_remote_copy(
                src_ref=o.at[:, pl.ds(to % blocks * kept, kept), to // blocks, lanes],
                dst_ref=out.at[:, :, me, lanes],
                send_sem=send_sem.at[1],
                recv_sem=recv_sem.at[1, chunk],
                device_id={"lon": to},
                device_id_type=MESH,
            ).start()

        if True:
            for at_z in range(zs):

                @pl.when(my_z == at_z)
                def _():
                    for offset in ranked(shape, at_z):
                        send_out(offset)

        pltpu.make_async_copy(
            o.at[:, pl.ds(me % blocks * kept, kept), me // blocks, lanes],
            out.at[:, :, me, lanes],
            recv_sem.at[1, chunk],
        ).start()

    for chunk in range(chunks):
        lanes = pl.ds(chunk * width, width)
        landed = out.at[:, :, :, lanes]
        pltpu.make_async_copy(landed, landed, recv_sem.at[1, chunk]).wait()
    sent = o.at[:, pl.ds(0, others)]
    pltpu.make_async_copy(sent, sent, send_sem.at[0]).wait()
    pltpu.make_async_copy(sent, sent, send_sem.at[1]).wait()


def solution(mesh):
    devices = mesh.shape["lon"]
    sizes = (4, devices // 8, 2, 2)

    def local(state):
        depth, fields, lats = state.shape
        chunks = sizes[3]
        kept = depth // 2
        first, second = tables(devices, depth)
        return pl.pallas_call(
            functools.partial(kernel, sizes),
            out_shape=jax.ShapeDtypeStruct((2, kept, fields, lats), jnp.float32),
            in_specs=[pl.BlockSpec(memory_space=pl.ANY)] * 3,
            out_specs=pl.BlockSpec(memory_space=pltpu.VMEM),
            scratch_shapes=[
                pltpu.VMEM((depth, fields, lats), jnp.float32),
                pltpu.VMEM((depth, devices, lats), jnp.float32),
                pltpu.VMEM((depth * devices, lats // chunks), jnp.float32),
                pltpu.VMEM((2, devices, kept, lats), jnp.float32),
                pltpu.VMEM(first.shape, jnp.bfloat16),
                pltpu.VMEM(second.shape, jnp.bfloat16),
                pltpu.SemaphoreType.DMA((2 + chunks,)),
                pltpu.SemaphoreType.DMA((2,)),
                pltpu.SemaphoreType.DMA((2, chunks)),
                pltpu.SemaphoreType.REGULAR((sizes[0] // 2 + sizes[1] // 2 - 1,)),
            ],
            compiler_params=pltpu.CompilerParams(
                collective_id=0, has_side_effects=True, vmem_limit_bytes=16 * 1024 * 1024
            ),
            name="spectrum",
        )(*(pltpu.with_memory_space_constraint(array, pltpu.HBM) for array in (state, jnp.asarray(first), jnp.asarray(second))))

    return jax.shard_map(
        local,
        mesh=mesh,
        in_specs=(P("lon", None, "lat"),),
        out_specs=P(None, "lon", None, "lat"),
        check_vma=False,
    )
```
